32 devices in a mesh: section: 1, grp: 16 (over z, x, core), tp: 2 (over y).
Axes of the slice: x: 2, y: 2, z: 4, core: 2. Of those that a mesh axis runs over, the one named last changes fastest.
Arguments:
- partials: bfloat16 [2, 1, 2048, 8192], P('tp', 'section', 'grp'), may hold values from -3 to 3
- residual: bfloat16 [1, 2048, 8192], P('section', 'grp', 'tp'), may hold values from -300 to 300
- norm_gain: bfloat16 [8192], replicated, may hold values from 0.099609375 to 1.8984375
- w_query: bfloat16 [8192, 8192], P('grp', ('section', 'tp')), may hold values from -0.0625 to 0.0625
- w_keyval: bfloat16 [8192, 2048], P('grp', ('section', 'tp')), may hold values from -0.0625 to 0.0625
- bias_query: bfloat16 [8192], P(('section', 'tp')), may hold values from -3 to 3
- bias_keyval: bfloat16 [2048], P(('section', 'tp')), may hold values from -3 to 3
Outputs:
- hidden: bfloat16 [1, 2048, 8192], P('section', 'grp', 'tp')
- query: bfloat16 [1, 2048, 8192], P(None, 'grp', ('section', 'tp'))
- keyval: bfloat16 [1, 2048, 2048], P(None, 'grp', ('section', 'tp'))
The draws below stay inside these ranges and needn't reach their ends.
All inputs are finite; a program needn't handle non-finite values.
Results may differ from the reference program's by a relative error of at most 0.01.
Values may be sent and summed in bfloat16 or wider, within the bound.
A program may use at most 192 MiB of HBM per device.

```python
import jax
import jax.numpy as jnp
from jax import lax

D = 8192
LEN = 2048
SEQS = 1
PARTS_SIZE = 2
QCOLS = 8192
KVCOLS = 2048


def draw_residual(key, part):
    base_key = jax.random.fold_in(key, 11)
    key_normal, key_jitter, key_rows = jax.random.split(base_key, 3)
    column_ramp = 10.0 ** (jnp.arange(D, dtype=jnp.float32) / D)
    column_jitter = jax.random.uniform(key_jitter, (D,), jnp.float32, 0.5, 1.5)
    normal_part = jnp.clip(jax.random.normal(key_normal, (SEQS, LEN, D), jnp.float32), -4.0, 4.0)
    row_scale = 10.0 ** jax.random.uniform(key_rows, (SEQS, LEN, 1), jnp.float32, 0.0, 1.0)
    values = 0.3 * normal_part * column_ramp * column_jitter * row_scale
    return values.astype(jnp.bfloat16)


def block_levels(key, dims, cuts, low, high):
    factor_of = 1.0
    for axis_at, parts in cuts:
        draws = jax.random.uniform(jax.random.fold_in(jax.random.fold_in(key, 6), axis_at), (parts,), jnp.float32, low / len(cuts), high / len(cuts))
        factor_of = factor_of * jnp.repeat(jnp.exp(draws), dims[axis_at] // parts).reshape((-1,) + (1,) * (len(dims) - 1 - axis_at))
    return factor_of


def bell_draw(key, dims, deviation, limit, shards=(), kind=jnp.bfloat16):
    entries = jax.random.normal(key, dims, jnp.float32) * deviation
    if len(shards) > 0:
        entries = block_levels(key, dims, shards, -0.22, 0.18) * entries
    return jnp.clip(entries, min=-limit, max=limit).astype(kind)


def setup_inputs(seed: int = 0) -> dict:
    keys = jax.random.split(jax.random.key(seed), 8)
    partials = bell_draw(keys[0], (PARTS_SIZE, SEQS, LEN, D), 0.5, 3.0, ((0, 2), (2, 16)))
    residual = draw_residual(jax.random.fold_in(keys[7], 71), 0)
    norm_gain = jnp.clip(1.0 + 0.18 * jax.random.normal(keys[2], (D,), jnp.float32), 0.099609375, 1.8984375).astype(jnp.bfloat16)
    w_query = bell_draw(keys[3], (D, QCOLS), D ** -0.5, 0.0625, ((0, 16), (1, 2)))
    w_keyval = bell_draw(keys[4], (D, KVCOLS), D ** -0.5, 0.0625, ((0, 16), (1, 2)))
    bias_query = bell_draw(keys[5], (QCOLS,), 0.5, 3.0, ((0, 2),))
    bias_keyval = bell_draw(keys[6], (KVCOLS,), 0.5, 3.0, ((0, 2),))
    return {"partials": partials, "residual": residual, "norm_gain": norm_gain, "w_query": w_query, "w_keyval": w_keyval, "bias_query": bias_query, "bias_keyval": bias_keyval}


epsilon = 1e-06

def reference(partials, residual, norm_gain, w_query, w_keyval, bias_query, bias_keyval):
    summed = jnp.zeros(residual.shape, jnp.float32)
    for part_index in range(PARTS_SIZE):
        summed = summed + partials[part_index].astype(jnp.float32)
    hidden = (residual.astype(jnp.float32) + summed).astype(jnp.bfloat16)
    widened = hidden.astype(jnp.float32)
    mean_square = lax.optimization_barrier(jnp.mean(widened * widened, axis=-1, keepdims=True))
    normed = (widened * lax.rsqrt(mean_square + epsilon) * norm_gain.astype(jnp.float32)).astype(jnp.bfloat16)
    flattened = normed.reshape(SEQS * LEN, D)
    query = jnp.dot(flattened, w_query, preferred_element_type=jnp.float32) + bias_query.astype(jnp.float32)
    keyval = jnp.dot(flattened, w_keyval, preferred_element_type=jnp.float32) + bias_keyval.astype(jnp.float32)
    query = query.astype(jnp.bfloat16).reshape(SEQS, LEN, QCOLS)
    keyval = keyval.astype(jnp.bfloat16).reshape(SEQS, LEN, KVCOLS)
    return (hidden, query, keyval)
```

```python
import jax
import jax.numpy as jnp
from jax import lax
from jax.sharding import PartitionSpec as P

epsilon = 1e-06


def local(partials, residual, norm_gain, w_query, w_keyval, bias_query, bias_keyval):
    model_width = norm_gain.shape[0]
    summed = lax.psum_scatter(
        partials[0], "tp", scatter_dimension=2, tiled=True
    ).astype(jnp.float32)
    hidden = (residual.astype(jnp.float32) + summed).astype(jnp.bfloat16)
    widened = hidden.astype(jnp.float32)
    squares = lax.psum(jnp.sum(widened * widened, axis=-1), "tp")
    feature_share = widened.shape[2]
    offset = lax.axis_index("tp") * feature_share
    local_gain = lax.dynamic_slice_in_dim(norm_gain, offset, feature_share, 0).astype(jnp.float32)
    scaled = (widened * local_gain).astype(jnp.bfloat16)
    scaled = lax.all_gather(scaled, "tp", axis=2, tiled=True)
    gathered_squares = lax.all_gather(squares, "section", axis=0, tiled=True)
    scale = lax.rsqrt(gathered_squares / model_width + epsilon)[..., None]
    exchanged = lax.all_to_all(scaled, "grp", split_axis=2, concat_axis=1, tiled=True)
    exchanged = lax.all_gather(exchanged, "section", axis=0, tiled=True)
    seqs, length, depth = exchanged.shape
    flat = exchanged.reshape(seqs * length, depth)

    def project(weight, bias):
        total = jnp.dot(flat, weight, preferred_element_type=jnp.float32).astype(jnp.bfloat16)
        total = total.reshape(seqs, length, -1)
        own = lax.psum_scatter(total, "grp", scatter_dimension=1, tiled=True)
        return (own.astype(jnp.float32) * scale + bias.astype(jnp.float32)).astype(jnp.bfloat16)

    keyval = project(w_keyval, bias_keyval)
    query = project(w_query, bias_query)
    return (hidden, query, keyval)


def solution(mesh):
    placed = (
        P("tp", "section", "grp", None),
        P("section", "grp", "tp"),
        P(),
        P("grp", ("section", "tp")),
        P("grp", ("section", "tp")),
        P(("section", "tp")),
        P(("section", "tp")),
    )
    return jax.shard_map(
        local,
        mesh=mesh,
        in_specs=placed,
        out_specs=(
            P("section", "grp", "tp"),
            P(None, "grp", ("section", "tp")),
            P(None, "grp", ("section", "tp")),
        ),
        check_vma=False,
    )
```

```python
import functools
import math

import jax
import jax.numpy as jnp
from jax import lax
from jax.experimental import pallas as pl
from jax.experimental.pallas import tpu as pltpu
from jax.sharding import PartitionSpec as P

epsilon = 1e-06
MESH = pl.DeviceIdType.MESH
CORES = 2
SIDES = 2


def kernel(ranks, width, rows_ref, wq_ref, wk_ref, scale_ref, bias_ref, query_ref, keyval_ref,
           xs, wide, side_out, side_in, rank_out, rank_in, own,
           w_local, w_send, w_recv, x_local, x_send, x_recv, s_send, s_recv, r_send, r_recv):
    me = lax.axis_index("grp")
    core = lax.rem(me, CORES)
    chip = me // CORES
    side = lax.rem(chip, SIDES)
    rank = chip // SIDES
    chips = ranks * SIDES
    mate = chip * CORES + (1 - core)
    depth, q_cols = wq_ref.shape
    k_cols = wk_ref.shape[1]
    share = CORES * depth
    steps = (q_cols + k_cols) // width

    def device(at_rank, at_side):
        return (at_rank * SIDES + at_side) * CORES + core

    barrier = pltpu.get_barrier_semaphore()
    pl.semaphore_signal(barrier, inc=1, device_id={"grp": mate}, device_id_type=MESH)
    for off in range(1, chips):
        to = lax.rem(chip + off, chips) * CORES + core
        pl.semaphore_signal(barrier, inc=1, device_id={"grp": to}, device_id_type=MESH)
    pl.semaphore_wait(barrier, chips)

    def x_copy(off):
        to = lax.rem(chip + off, chips)
        return pltpu.make_async_remote_copy(
            src_ref=rows_ref.at[:, pl.ds(pl.multiple_of(to * share, share), share)],
            dst_ref=xs.at[chip],
            send_sem=x_send.at[off], recv_sem=x_recv.at[chip],
            device_id={"grp": to * CORES + core}, device_id_type=MESH)

    def x_wait(source):
        pltpu.make_async_remote_copy(
            src_ref=rows_ref.at[:, pl.ds(0, share)], dst_ref=xs.at[source],
            send_sem=x_send.at[0], recv_sem=x_recv.at[source],
            device_id={"grp": mate}, device_id_type=MESH).wait_recv()

    x_own = pltpu.make_async_copy(
        rows_ref.at[:, pl.ds(pl.multiple_of(chip * share, share), share)], xs.at[chip], x_local)
    x_own.start()
    offsets = list(range(1, chips))
    for off in offsets:
        x_copy(off).start()

    mine = pl.ds(pl.multiple_of(core * depth, depth), depth)
    q_part = wide.at[mine, pl.ds(0, q_cols)]
    k_part = wide.at[mine, pl.ds(q_cols, k_cols)]
    locals_ = [pltpu.make_async_copy(wq_ref, q_part, w_local.at[0]),
               pltpu.make_async_copy(wk_ref, k_part, w_local.at[1])]
    sends = [pltpu.make_async_remote_copy(
        src_ref=src, dst_ref=dst, send_sem=w_send.at[i], recv_sem=w_recv.at[i],
        device_id={"grp": mate}, device_id_type=MESH)
        for i, (src, dst) in enumerate(((wq_ref, q_part), (wk_ref, k_part)))]
    for copy in sends + locals_:
        copy.start()
    for copy in locals_:
        copy.wait()
    theirs = pl.ds(pl.multiple_of((1 - core) * depth, depth), depth)
    for i, (src, dst) in enumerate(((wq_ref, wide.at[theirs, pl.ds(0, q_cols)]),
                                    (wk_ref, wide.at[theirs, pl.ds(q_cols, k_cols)]))):
        pltpu.make_async_remote_copy(
            src_ref=src, dst_ref=dst, send_sem=w_send.at[i], recv_sem=w_recv.at[i],
            device_id={"grp": mate}, device_id_type=MESH).wait_recv()
    x_own.wait()

    def columns(j):
        return pl.ds(pl.multiple_of(j * width, width), width)

    def s_copy(k, j):
        return pltpu.make_async_remote_copy(
            src_ref=side_out.at[k, :, columns(j)], dst_ref=side_in.at[k, :, columns(j)],
            send_sem=s_send.at[k, j], recv_sem=s_recv.at[k, j],
            device_id={"grp": device(rank, 1 - side)}, device_id_type=MESH)

    def r_copy(k, j):
        return pltpu.make_async_remote_copy(
            src_ref=rank_out.at[k, :, columns(j)], dst_ref=rank_in.at[k, :, columns(j)],
            send_sem=r_send.at[k, j], recv_sem=r_recv.at[k, j],
            device_id={"grp": device(lax.rem(rank + k, ranks), side)}, device_id_type=MESH)

    order = list(range(1, ranks)) + [0]
    for k in order:
        source = lax.rem(rank + k, ranks) * SIDES + (1 - side)
        x_wait(source)

        def body(j, carry, k=k, source=source):
            side_out[k, :, columns(j)] = jnp.dot(
                xs[source], wide[:, columns(j)], preferred_element_type=jnp.float32
            ).astype(jnp.bfloat16)
            s_copy(k, j).start()
            return carry

        lax.fori_loop(0, steps, body, 0)
    for k in order:
        source = lax.rem(rank + k, ranks) * SIDES + side
        if k:
            x_wait(source)

        def body(j, carry, k=k, source=source):
            total = jnp.dot(xs[source], wide[:, columns(j)], preferred_element_type=jnp.float32)
            s_copy(k, j).wait_recv()
            total = total + side_in[k, :, columns(j)].astype(jnp.float32)
            if k:
                rank_out[k, :, columns(j)] = total.astype(jnp.bfloat16)
                r_copy(k, j).start()
            else:
                own[:, columns(j)] = total
            return carry

        lax.fori_loop(0, steps, body, 0)

    def finish(first, count, out_ref):
        def body(i, carry):
            j = first + i
            total = own[:, columns(j)]
            for k in range(1, ranks):
                r_copy(k, j).wait_recv()
                total = total + rank_in[k, :, columns(j)].astype(jnp.float32)
            total = total * scale_ref[...] + bias_ref[:, columns(j)]
            out_ref[:, columns(i)] = total.astype(jnp.bfloat16)
            return carry

        lax.fori_loop(0, count, body, 0)

    finish(0, q_cols // width, query_ref)
    finish(q_cols // width, k_cols // width, keyval_ref)

    for copy in sends:
        copy.wait_send()
    for off in offsets:
        x_copy(off).wait_send()

    def drain(j, carry):
        for k in range(ranks):
            s_copy(k, j).wait_send()
            if k:
                r_copy(k, j).wait_send()
        return carry

    lax.fori_loop(0, steps, drain, 0)


def project(rows, w_query, w_keyval, scale, bias, group):
    count = rows.shape[0]
    depth, q_cols = w_query.shape
    k_cols = w_keyval.shape[1]
    total = q_cols + k_cols
    width = math.gcd(math.gcd(q_cols, k_cols), 512)
    steps = total // width
    ranks = group // (CORES * SIDES)
    chips = group // CORES
    share = CORES * depth
    vmem = pl.BlockSpec(memory_space=pltpu.VMEM)
    hbm = pl.BlockSpec(memory_space=pl.ANY)
    dma = pltpu.SemaphoreType.DMA
    return pl.pallas_call(
        functools.partial(kernel, ranks, width),
        out_shape=(jax.ShapeDtypeStruct((count, q_cols), jnp.bfloat16),
                   jax.ShapeDtypeStruct((count, k_cols), jnp.bfloat16)),
        in_specs=[vmem, hbm, hbm, vmem, vmem],
        out_specs=(vmem, vmem),
        scratch_shapes=[
            pltpu.VMEM((chips, count, share), jnp.bfloat16),
            pltpu.VMEM((share, total), jnp.bfloat16),
            pltpu.VMEM((ranks, count, total), jnp.bfloat16),
            pltpu.VMEM((ranks, count, total), jnp.bfloat16),
            pltpu.VMEM((ranks, count, total), jnp.bfloat16),
            pltpu.VMEM((ranks, count, total), jnp.bfloat16),
            pltpu.VMEM((count, total), jnp.float32),
            dma((2,)), dma((2,)), dma((2,)),
            dma, dma((chips,)), dma((chips,)),
            dma((ranks, steps)), dma((ranks, steps)),
            dma((ranks, steps)), dma((ranks, steps)),
        ],
        compiler_params=pltpu.CompilerParams(
            collective_id=0, has_side_effects=True, vmem_limit_bytes=60 * 1024 * 1024),
    )(rows, w_query, w_keyval, scale, bias)


def local(group, partials, residual, norm_gain, w_query, w_keyval, bias_query, bias_keyval):
    model_width = norm_gain.shape[0]
    summed = lax.psum_scatter(
        partials[0], "tp", scatter_dimension=2, tiled=True
    ).astype(jnp.float32)
    hidden = (residual.astype(jnp.float32) + summed).astype(jnp.bfloat16)
    widened = hidden.astype(jnp.float32)
    squares = lax.psum(jnp.sum(widened * widened, axis=-1), "tp")
    feature_share = widened.shape[2]
    offset = lax.axis_index("tp") * feature_share
    local_gain = lax.dynamic_slice_in_dim(norm_gain, offset, feature_share, 0).astype(jnp.float32)
    scaled = (widened * local_gain).astype(jnp.bfloat16)
    scaled = lax.all_gather(scaled, "tp", axis=2, tiled=True)
    scaled = lax.all_gather(scaled, "section", axis=0, tiled=True)
    squares = lax.all_gather(squares, "section", axis=0, tiled=True)
    seqs, length = squares.shape
    scale = lax.rsqrt(squares / model_width + epsilon).reshape(-1, 1)
    bias = jnp.concatenate([bias_query, bias_keyval]).astype(jnp.float32)[None]
    query, keyval = project(
        scaled.reshape(seqs * length, model_width), w_query, w_keyval, scale, bias, group)
    return (hidden, query.reshape(seqs, length, -1), keyval.reshape(seqs, length, -1))


def solution(mesh):
    placed = (
        P("tp", "section", "grp", None),
        P("section", "grp", "tp"),
        P(),
        P("grp", ("section", "tp")),
        P("grp", ("section", "tp")),
        P(("section", "tp")),
        P(("section", "tp")),
    )
    return jax.shard_map(
        functools.partial(local, mesh.shape["grp"]),
        mesh=mesh,
        in_specs=placed,
        out_specs=(
            P("section", "grp", "tp"),
            P(None, "grp", ("section", "tp")),
            P(None, "grp", ("section", "tp")),
        ),
        check_vma=False,
    )
```

```python
import functools
import math

import jax
import jax.numpy as jnp
from jax import lax
from jax.experimental import pallas as pl
from jax.experimental.pallas import tpu as pltpu
from jax.sharding import PartitionSpec as P

epsilon = 1e-06
MESH = pl.DeviceIdType.MESH
CORES = 2
SIDES = 2


def kernel(ranks, parts, width, rows_ref, wq_ref, wk_ref, square_ref, bias_ref,
           query_ref, keyval_ref, xs, wide, side_out, side_in, rank_out, rank_in, own, squares,
           w_local, w_send, w_recv, x_local, x_send, x_recv, f_send, f_recv, q_send, q_recv,
           s_send, s_recv, r_send, r_recv):
    me = lax.axis_index("grp")
    part = lax.axis_index("tp")
    core = lax.rem(me, CORES)
    chip = me // CORES
    side = lax.rem(chip, SIDES)
    rank = chip // SIDES
    chips = ranks * SIDES
    mate = chip * CORES + (1 - core)
    depth, q_cols = wq_ref.shape
    k_cols = wk_ref.shape[1]
    share = CORES * depth
    steps = (q_cols + k_cols) // width

    def device(at_rank, at_side):
        return (at_rank * SIDES + at_side) * CORES + core

    barrier = pltpu.get_barrier_semaphore()
    pl.semaphore_signal(barrier, inc=1, device_id={"grp": mate}, device_id_type=MESH)
    for d in range(parts):
        for off in range(chips):
            if d or off:
                to = lax.rem(chip + off, chips) * CORES + core
                pl.semaphore_signal(
                    barrier, inc=1, device_id={"grp": to, "tp": lax.rem(part + d, parts)},
                    device_id_type=MESH)
    pl.semaphore_wait(barrier, chips * parts)

    held = chips // parts
    piece = rows_ref.shape[0] // parts
    whole_here = chip // held == part

    def piece_of(index):
        return pl.ds(pl.multiple_of(index * piece, piece), piece)

    def x_ends(i, d):
        rows = piece_of(lax.rem(part + d, parts))
        return rows_ref.at[rows, pl.ds(i * share, share)], xs.at[chip, rows]

    def x_copy(i, d):
        src, dst = x_ends(i, d)
        return pltpu.make_async_remote_copy(
            src_ref=src, dst_ref=dst, send_sem=x_send.at[i, d], recv_sem=x_recv.at[chip],
            device_id={"grp": (part * held + i) * CORES + core, "tp": lax.rem(part + d, parts)},
            device_id_type=MESH)

    def x_own(i):
        src, dst = x_ends(i, 0)
        return pltpu.make_async_copy(src, dst, x_local)

    def each_x(far, near):
        for i in range(held):
            here = jnp.logical_and(whole_here, lax.rem(chip, held) == i)
            pl.when(here)(functools.partial(near, i))
            pl.when(jnp.logical_not(here))(functools.partial(far, i, 0))
            for d in range(1, parts):
                far(i, d)

    each_x(lambda i, d: x_copy(i, d).start(), lambda i: x_own(i).start())

    def q_copy(d):
        return pltpu.make_async_remote_copy(
            src_ref=square_ref, dst_ref=squares.at[d],
            send_sem=q_send.at[d], recv_sem=q_recv.at[d],
            device_id={"tp": lax.rem(part + d, parts)}, device_id_type=MESH)

    for d in range(1, parts):
        q_copy(d).start()

    def x_arrive(source):
        pltpu.make_async_remote_copy(
            src_ref=xs.at[source, piece_of(part)], dst_ref=xs.at[source, piece_of(part)],
            send_sem=x_send.at[0, 0], recv_sem=x_recv.at[source],
            device_id={"grp": mate}, device_id_type=MESH).wait_recv()

    def f_copy(source, d):
        return pltpu.make_async_remote_copy(
            src_ref=xs.at[source, piece_of(part)], dst_ref=xs.at[source, piece_of(part)],
            send_sem=f_send.at[source, d], recv_sem=f_recv.at[source, d],
            device_id={"tp": lax.rem(part + d, parts)}, device_id_type=MESH)

    def pass_on(source, here):
        if here:
            def near():
                for i in range(held):
                    pl.when(lax.rem(chip, held) == i)(lambda i=i: x_own(i).wait())

            pl.when(whole_here)(near)
            pl.when(jnp.logical_not(whole_here))(lambda: x_arrive(source))
        else:
            x_arrive(source)
        for d in range(1, parts):
            f_copy(source, d).start()

    def x_wait(source):
        for d in range(1, parts):
            rows = piece_of(lax.rem(part + parts - d, parts))
            pltpu.make_async_remote_copy(
                src_ref=xs.at[source, rows], dst_ref=xs.at[source, rows],
                send_sem=f_send.at[source, d], recv_sem=f_recv.at[source, d],
                device_id={"grp": mate}, device_id_type=MESH).wait_recv()

    mine = pl.ds(pl.multiple_of(core * depth, depth), depth)
    q_part = wide.at[mine, pl.ds(0, q_cols)]
    k_part = wide.at[mine, pl.ds(q_cols, k_cols)]
    locals_ = [pltpu.make_async_copy(wq_ref, q_part, w_local.at[0]),
               pltpu.make_async_copy(wk_ref, k_part, w_local.at[1])]
    sends = [pltpu.make_async_remote_copy(
        src_ref=src, dst_ref=dst, send_sem=w_send.at[i], recv_sem=w_recv.at[i],
        device_id={"grp": mate}, device_id_type=MESH)
        for i, (src, dst) in enumerate(((wq_ref, q_part), (wk_ref, k_part)))]
    for copy in sends + locals_:
        copy.start()
    for copy in locals_:
        copy.wait()
    theirs = pl.ds(pl.multiple_of((1 - core) * depth, depth), depth)
    for i, (src, dst) in enumerate(((wq_ref, wide.at[theirs, pl.ds(0, q_cols)]),
                                    (wk_ref, wide.at[theirs, pl.ds(q_cols, k_cols)]))):
        pltpu.make_async_remote_copy(
            src_ref=src, dst_ref=dst, send_sem=w_send.at[i], recv_sem=w_recv.at[i],
            device_id={"grp": mate}, device_id_type=MESH).wait_recv()

    def columns(j):
        return pl.ds(pl.multiple_of(j * width, width), width)

    def s_copy(k, j):
        return pltpu.make_async_remote_copy(
            src_ref=side_out.at[k, :, columns(j)], dst_ref=side_in.at[k, :, columns(j)],
            send_sem=s_send.at[k, j], recv_sem=s_recv.at[k, j],
            device_id={"grp": device(rank, 1 - side)}, device_id_type=MESH)

    def r_copy(k, j):
        return pltpu.make_async_remote_copy(
            src_ref=rank_out.at[k, :, columns(j)], dst_ref=rank_in.at[k, :, columns(j)],
            send_sem=r_send.at[k, j], recv_sem=r_recv.at[k, j],
            device_id={"grp": device(lax.rem(rank + k, ranks), side)}, device_id_type=MESH)

    order = list(range(1, ranks)) + [0]
    for k in order:
        source = lax.rem(rank + k, ranks) * SIDES + (1 - side)
        pass_on(source, False)
        pass_on(lax.rem(rank + k, ranks) * SIDES + side, k == 0)
        x_wait(source)

        def body(j, carry, k=k, source=source):
            side_out[k, :, columns(j)] = jnp.dot(
                xs[source], wide[:, columns(j)], preferred_element_type=jnp.float32
            ).astype(jnp.bfloat16)
            s_copy(k, j).start()
            return carry

        lax.fori_loop(0, steps, body, 0)
    for k in order:
        source = lax.rem(rank + k, ranks) * SIDES + side
        x_wait(source)

        def body(j, carry, k=k, source=source):
            total = jnp.dot(xs[source], wide[:, columns(j)], preferred_element_type=jnp.float32)
            s_copy(k, j).wait_recv()
            total = total + side_in[k, :, columns(j)].astype(jnp.float32)
            if k:
                rank_out[k, :, columns(j)] = total.astype(jnp.bfloat16)
                r_copy(k, j).start()
            else:
                own[:, columns(j)] = total
            return carry

        lax.fori_loop(0, steps, body, 0)

    mean_square = square_ref[...]
    for d in range(1, parts):
        q_copy(d).wait_recv()
        mean_square = mean_square + squares[d]
    model_width = rows_ref.shape[1] * parts
    scale = lax.rsqrt(mean_square[:, :1] / model_width + epsilon)

    def finish(first, count, out_ref):
        def body(i, carry):
            j = first + i
            total = own[:, columns(j)]
            for k in range(1, ranks):
                r_copy(k, j).wait_recv()
                total = total + rank_in[k, :, columns(j)].astype(jnp.float32)
            total = total * scale + bias_ref[:, columns(j)]
            out_ref[:, columns(i)] = total.astype(jnp.bfloat16)
            return carry

        lax.fori_loop(0, count, body, 0)

    finish(0, q_cols // width, query_ref)
    finish(q_cols // width, k_cols // width, keyval_ref)

    for copy in sends:
        copy.wait_send()
    each_x(lambda i, d: x_copy(i, d).wait_send(), lambda i: None)
    for d in range(1, parts):
        q_copy(d).wait_send()
        for source in range(chips):
            f_copy(source, d).wait_send()

    def drain(j, carry):
        for k in range(ranks):
            s_copy(k, j).wait_send()
            if k:
                r_copy(k, j).wait_send()
        return carry

    lax.fori_loop(0, steps, drain, 0)


def project(rows, w_query, w_keyval, squares, bias, group, parts):
    count = rows.shape[0]
    depth, q_cols = w_query.shape
    k_cols = w_keyval.shape[1]
    total = q_cols + k_cols
    width = math.gcd(math.gcd(q_cols, k_cols), 512)
    steps = total // width
    ranks = group // (CORES * SIDES)
    chips = group // CORES
    share = CORES * depth
    vmem = pl.BlockSpec(memory_space=pltpu.VMEM)
    hbm = pl.BlockSpec(memory_space=pl.ANY)
    dma = pltpu.SemaphoreType.DMA
    return pl.pallas_call(
        functools.partial(kernel, ranks, parts, width),
        out_shape=(jax.ShapeDtypeStruct((count, q_cols), jnp.bfloat16),
                   jax.ShapeDtypeStruct((count, k_cols), jnp.bfloat16)),
        in_specs=[vmem, hbm, hbm, vmem, vmem],
        out_specs=(vmem, vmem),
        scratch_shapes=[
            pltpu.VMEM((chips, count, share), jnp.bfloat16),
            pltpu.VMEM((share, total), jnp.bfloat16),
            pltpu.VMEM((ranks, count, total), jnp.bfloat16),
            pltpu.VMEM((ranks, count, total), jnp.bfloat16),
            pltpu.VMEM((ranks, count, total), jnp.bfloat16),
            pltpu.VMEM((ranks, count, total), jnp.bfloat16),
            pltpu.VMEM((count, total), jnp.float32),
            pltpu.VMEM((parts, count, squares.shape[1]), jnp.float32),
            dma((2,)), dma((2,)), dma((2,)),
            dma, dma((chips // parts, parts)), dma((chips,)),
            dma((chips, parts)), dma((chips, parts)), dma((parts,)), dma((parts,)),
            dma((ranks, steps)), dma((ranks, steps)),
            dma((ranks, steps)), dma((ranks, steps)),
        ],
        compiler_params=pltpu.CompilerParams(
            collective_id=0, has_side_effects=True, vmem_limit_bytes=60 * 1024 * 1024),
    )(rows, w_query, w_keyval, squares, bias)


def own_sum(partial, feature_share, parts):
    if parts != 2:
        return lax.psum_scatter(
            partial, "tp", scatter_dimension=2, tiled=True).astype(jnp.float32)
    part = lax.axis_index("tp")
    own = lax.dynamic_slice_in_dim(partial, part * feature_share, feature_share, 2)
    other = lax.dynamic_slice_in_dim(partial, (1 - part) * feature_share, feature_share, 2)
    other = lax.ppermute(other, "tp", [(0, 1), (1, 0)])
    return own.astype(jnp.float32) + other.astype(jnp.float32)


def local(group, parts, partials, residual, norm_gain, w_query, w_keyval, bias_query, bias_keyval):
    feature_share = residual.shape[2]
    summed = own_sum(partials[0], feature_share, parts)
    hidden = (residual.astype(jnp.float32) + summed).astype(jnp.bfloat16)
    widened = hidden.astype(jnp.float32)
    squares = jnp.sum(widened * widened, axis=-1)
    offset = lax.axis_index("tp") * feature_share
    local_gain = lax.dynamic_slice_in_dim(norm_gain, offset, feature_share, 0).astype(jnp.float32)
    scaled = (widened * local_gain).astype(jnp.bfloat16)
    scaled = lax.all_gather(scaled, "section", axis=0, tiled=True)
    squares = lax.all_gather(squares, "section", axis=0, tiled=True)
    seqs, length = squares.shape
    squares = jnp.broadcast_to(squares.reshape(-1, 1), (seqs * length, 128))
    bias = jnp.concatenate([bias_query, bias_keyval]).astype(jnp.float32)[None]
    query, keyval = project(
        scaled.reshape(seqs * length, feature_share), w_query, w_keyval, squares, bias,
        group, parts)
    return (hidden, query.reshape(seqs, length, -1), keyval.reshape(seqs, length, -1))


def solution(mesh):
    placed = (
        P("tp", "section", "grp", None),
        P("section", "grp", "tp"),
        P(),
        P("grp", ("section", "tp")),
        P("grp", ("section", "tp")),
        P(("section", "tp")),
        P(("section", "tp")),
    )
    return jax.shard_map(
        functools.partial(local, mesh.shape["grp"], mesh.shape["tp"]),
        mesh=mesh,
        in_specs=placed,
        out_specs=(
            P("section", "grp", "tp"),
            P(None, "grp", ("section", "tp")),
            P(None, "grp", ("section", "tp")),
        ),
        check_vma=False,
    )
```
